32 devices in a mesh: grp: 4 (over x, core), sub: 8 (over z, y).
Axes of the slice: x: 2, y: 2, z: 4, core: 2. Of those that a mesh axis runs over, the one named last changes fastest.
Arguments:
- snapshots: bfloat16 [2048, 2, 32, 128], P(None, None, ('grp', 'sub')), may hold values from -6 to 6
- steering: bfloat16 [32, 2, 128, 64], P(('grp', 'sub')), may hold values from -0.375 to 0.375
- combining: bfloat16 [32, 2, 64, 1024], P(('grp', 'sub')), may hold values from -0.09375 to 0.09375
- beam_list: int32 [1024], replicated, may hold values from 0 to 1023, each once
Outputs:
- beams_out: bfloat16 [2, 2048, 1024], P(None, ('grp', 'sub'))
The draws below stay inside these ranges and needn't reach their ends.
Inputs may be any that keep to these rules, and one draw needn't show every extreme that they name: `beam_list`: each of the 1024 beams appears once.
All inputs are finite; a program needn't handle non-finite values.
Results may differ from the reference program's by a relative error of at most 0.0065.
Values may be sent and summed in bfloat16 or wider, within the bound.
A program may use at most 128 MiB of HBM per device.

```python
import jax
import jax.numpy as jnp
from jax import lax

EL = 128
PB = 64
NBEAM = 1024
SNAP = 2048
SUBS = 32


def level_of(stream_key, extent, pieces, smallest, largest):
    def one(dim, blocks):
        draws = jax.random.uniform(jax.random.fold_in(jax.random.fold_in(stream_key, 6), dim), (blocks,), jnp.float32, smallest / len(pieces), largest / len(pieces))
        return jnp.repeat(jnp.exp(draws), extent[dim] // blocks).reshape((-1,) + (1,) * (len(extent) - dim - 1))

    factor_of = one(*pieces[0])
    for cut in pieces[1:]:
        factor_of = factor_of * one(*cut)
    return factor_of


def noise(rng, dims, width, limit, shards=(), kind=jnp.bfloat16):
    result = jax.random.normal(rng, dims, jnp.float32) * width
    if len(shards) > 0:
        result = level_of(rng, dims, shards, -0.22, 0.18) * result
    return jnp.clip(result, min=-limit, max=limit).astype(kind)


def setup_inputs(seed: int = 0) -> dict:
    keys = jax.random.split(jax.random.key(seed), 5)
    return {
        "snapshots": noise(keys[0], (SNAP, 2, SUBS, EL), 1.0, 6.0, ((2, 32),)),
        "steering": noise(keys[1], (SUBS, 2, EL, PB), (2 * EL) ** -0.5, 0.375, ((0, 32),)),
        "combining": noise(keys[2], (SUBS, 2, PB, NBEAM), (2 * SUBS * PB) ** -0.5, 0.09375, ((0, 32),)),
        "beam_list": jax.random.permutation(keys[3], NBEAM).astype(jnp.int32),
    }


def reference(snapshots, steering, combining, beam_list):
    ordered = jnp.take(combining, beam_list, axis=3)

    def accumulate(subarray, running):
        signal = lax.dynamic_index_in_dim(snapshots, subarray, 2, keepdims=False).astype(jnp.float32)
        steer_s = lax.dynamic_index_in_dim(steering, subarray, 0, keepdims=False).astype(jnp.float32)
        comb_s = lax.dynamic_index_in_dim(ordered, subarray, 0, keepdims=False).astype(jnp.float32)
        sig_real = signal[:, 0]
        sig_imag = signal[:, 1]
        beam_real = jnp.dot(sig_real, steer_s[0]) - jnp.dot(sig_imag, steer_s[1])
        beam_imag = jnp.dot(sig_real, steer_s[1]) + jnp.dot(sig_imag, steer_s[0])
        beam_real = lax.optimization_barrier(beam_real.astype(jnp.bfloat16)).astype(jnp.float32)
        beam_imag = lax.optimization_barrier(beam_imag.astype(jnp.bfloat16)).astype(jnp.float32)
        final_real = jnp.dot(beam_real, comb_s[0]) - jnp.dot(beam_imag, comb_s[1])
        final_imag = jnp.dot(beam_real, comb_s[1]) + jnp.dot(beam_imag, comb_s[0])
        return running + jnp.stack([final_real, final_imag])

    running = lax.fori_loop(0, SUBS, accumulate, jnp.zeros((2, SNAP, NBEAM), jnp.float32))
    return running.astype(jnp.bfloat16)
```

```python
import functools

import jax
import jax.numpy as jnp
from jax import lax
from jax.experimental import pallas as pl
from jax.experimental.pallas import tpu as pltpu
from jax.sharding import PartitionSpec as P

MESH = pl.DeviceIdType.MESH
F32 = jnp.float32
BF16 = jnp.bfloat16


class Plan:
    def __init__(self, mesh, snap, width, beams):
        self.grp = mesh.shape["grp"]
        self.sub = mesh.shape["sub"]
        self.cores = 2 if self.grp % 2 == 0 else 1
        self.nx = self.grp // self.cores
        self.hi = self.grp if self.sub % self.grp == 0 else 1
        self.lo = self.sub // self.hi
        self.block = snap // (self.grp * self.sub)
        self.width = width
        self.beams = beams
        self.chunks = 4 if beams % 512 == 0 else 1
        self.cols = beams // self.chunks
        self.offsets = [(dx, dy) for dx in range(self.nx) for dy in range(self.lo)]
        self.slots = len(self.offsets) * self.cores


def beam_kernel(
    plan,
    x_ref,
    s_ref,
    w_ref,
    list_ref,
    out_ref,
    even_buf,
    odd_buf,
    pall,
    pbuf,
    lhs_buf,
    wbuf,
    own_buf,
    share_buf,
    got_buf,
    pick_buf,
    acc_buf,
    psend,
    precv,
    wsend,
    wrecv,
    ssend,
    srecv,
):
    cores, nx, lo, hi = plan.cores, plan.nx, plan.lo, plan.hi
    cols, width, block = plan.cols, plan.width, plan.block
    half = width // 2
    offsets = plan.offsets
    count = len(offsets)
    g = lax.axis_index("grp")
    s = lax.axis_index("sub")
    core, xi = lax.rem(g, cores), lax.div(g, cores)
    z, y = lax.div(s, lo), lax.rem(s, lo)

    def peer(dx, dy, dc):
        gg = lax.rem(xi + dx, nx) * cores + lax.rem(core + dc, cores)
        yy = lax.rem(y + dy, lo)
        return gg, yy

    def slot(o, dc):
        return dc * count + o

    plane = [(o, dc) for o in range(count) for dc in range(cores) if (o, dc) != (0, 0)]
    plane.sort(key=lambda item: -sum(1 for v in offsets[item[0]] if v))

    barrier = pltpu.get_barrier_semaphore()
    for o, dc in plane:
        gg, yy = peer(*offsets[o], dc)
        pl.semaphore_signal(barrier, inc=1, device_id=(gg, z * lo + yy), device_id_type=MESH)
    for dz in range(1, hi):
        pl.semaphore_signal(
            barrier, inc=1, device_id=(g, lax.rem(z + dz, hi) * lo + y), device_id_type=MESH
        )
    pl.semaphore_wait(barrier, len(plane) + hi - 1)

    def w_columns(c):
        return w_ref.at[:, pl.ds(c * cols, cols)]

    sends = []

    def send_w(c):
        for o in sorted(range(count), key=lambda o: -sum(1 for v in offsets[o] if v)):
            if o == 0:
                if cores > 1:
                    gg, yy = peer(0, 0, 1)
                    k = slot(0, 1)
                else:
                    continue
            else:
                gg, yy = peer(*offsets[o], 0)
                k = slot(o, 0)
            copy = pltpu.make_async_remote_copy(
                src_ref=w_columns(c),
                dst_ref=wbuf.at[c, k],
                send_sem=wsend.at[c, k],
                recv_sem=wrecv.at[c, k],
                device_id=(gg, z * lo + yy),
                device_id_type=MESH,
            )
            copy.start()
            sends.append(copy)

    def relay_w(c):
        if cores == 1:
            return
        gg, yy = peer(0, 0, 1)
        for o in range(1, count):
            wait_w(c, slot(o, 0))
            copy = pltpu.make_async_remote_copy(
                src_ref=wbuf.at[c, slot(o, 0)],
                dst_ref=wbuf.at[c, slot(o, 1)],
                send_sem=wsend.at[c, slot(o, 1)],
                recv_sem=wrecv.at[c, slot(o, 1)],
                device_id=(gg, z * lo + yy),
                device_id_type=MESH,
            )
            copy.start()
            sends.append(copy)

    def wait_w(c, k):
        pltpu.make_async_copy(wbuf.at[c, k], wbuf.at[c, k], wrecv.at[c, k]).wait()

    send_w(0)

    upper = s_ref[...]
    lower = jnp.concatenate([-upper[half:], upper[:half]], axis=0)
    rows_g = hi * lo * block
    contract = (((1,), (1,)), ((), ()))
    for gg in range(plan.grp):
        part = x_ref[pl.ds(gg * rows_g * 2, rows_g * 2), :]
        even_buf[...] = lax.dot_general(part, upper, contract, preferred_element_type=F32)
        odd_buf[...] = lax.dot_general(part, lower, contract, preferred_element_type=F32)
        value = even_buf[pl.ds(0, rows_g, stride=2), :] + odd_buf[pl.ds(1, rows_g, stride=2), :]
        pall[gg] = value.reshape(hi, lo, block, width).astype(BF16)

    for o, dc in plane:
        gg, yy = peer(*offsets[o], dc)
        k = slot(o, dc)
        copy = pltpu.make_async_remote_copy(
            src_ref=pall.at[gg, :, yy],
            dst_ref=pbuf.at[k],
            send_sem=psend.at[k],
            recv_sem=precv.at[k],
            device_id=(gg, z * lo + yy),
            device_id_type=MESH,
        )
        copy.start()
        sends.append(copy)

    for c in range(1, plan.chunks):
        send_w(c)

    for c in range(plan.chunks):
        row = lax.broadcasted_iota(jnp.int32, (cols, plan.beams), 0) + c * cols
        pick_buf[pl.ds(c * cols, cols), :] = jnp.where(row == list_ref[...], 1.0, 0.0).astype(BF16)
        wbuf[c, 0] = w_ref[:, pl.ds(c * cols, cols)]

    lhs_buf[:, pl.ds(0, width)] = pall[g, :, y].reshape(hi * block, width)
    relay_w(0)
    for o, dc in reversed(plane):
        k = slot(o, dc)
        pltpu.make_async_copy(pbuf.at[k], pbuf.at[k], precv.at[k]).wait()
        lhs_buf[:, pl.ds(k * width, width)] = pbuf[k].reshape(hi * block, width)

    def finish(c):
        total = own_buf[c, z]
        for dz in range(1, hi):
            pltpu.make_async_copy(got_buf.at[c, dz], got_buf.at[c, dz], srecv.at[c, dz]).wait()
            total = total + got_buf[c, dz].astype(F32)
        rounded = total.astype(BF16).reshape(2 * block, cols)
        placed = jnp.dot(rounded, pick_buf[pl.ds(c * cols, cols), :], preferred_element_type=F32)
        if c == 0:
            acc_buf[...] = placed
        else:
            acc_buf[...] += placed

    for c in range(plan.chunks):
        if c + 1 < plan.chunks:
            pass
        if cores > 1:
            for o in range(count):
                wait_w(c, slot(o, 1))
        else:
            for o in range(1, count):
                wait_w(c, slot(o, 0))
        weights = wbuf[c]
        w_real, w_imag = weights[:, :half], weights[:, half:]
        for part, rhs in enumerate(((w_real, -w_imag), (w_imag, w_real))):
            rhs = jnp.concatenate(rhs, axis=1).reshape(plan.slots * width, cols)
            value = jnp.dot(lhs_buf[...], rhs, preferred_element_type=F32)
            value = value.reshape(hi, block, cols)
            own_buf[c, :, part] = value
            share_buf[c, :, part] = value.astype(BF16)
        for dz in range(1, hi):
            zz = lax.rem(z + dz, hi)
            copy = pltpu.make_async_remote_copy(
                src_ref=share_buf.at[c, zz],
                dst_ref=got_buf.at[c, dz],
                send_sem=ssend.at[c, dz],
                recv_sem=srecv.at[c, dz],
                device_id=(g, zz * lo + y),
                device_id_type=MESH,
            )
            copy.start()
            sends.append(copy)
        if c + 1 < plan.chunks:
            relay_w(c + 1)
    for c in range(plan.chunks):
        finish(c)
    out_ref[...] = acc_buf[...].astype(BF16).reshape(2, block, plan.beams)
    for copy in sends:
        copy.wait_send()


def shards(plan, snapshots, steering, combining, beam_list):
    snap, _, _, elements = snapshots.shape
    signal = snapshots.reshape(snap * 2, elements)
    steer = jnp.transpose(steering[0], (0, 2, 1)).reshape(plan.width, elements)
    weights = combining.reshape(plan.width, plan.beams)
    rows_g = plan.hi * plan.lo * plan.block
    vmem = pl.BlockSpec(memory_space=pltpu.VMEM)
    dma = pltpu.SemaphoreType.DMA
    return pl.pallas_call(
        functools.partial(beam_kernel, plan),
        out_shape=jax.ShapeDtypeStruct((2, plan.block, plan.beams), BF16),
        in_specs=[vmem] * 4,
        out_specs=vmem,
        scratch_shapes=[
            pltpu.VMEM((rows_g * 2, plan.width), F32),
            pltpu.VMEM((rows_g * 2, plan.width), F32),
            pltpu.VMEM((plan.grp, plan.hi, plan.lo, plan.block, plan.width), BF16),
            pltpu.VMEM((plan.slots, plan.hi, plan.block, plan.width), BF16),
            pltpu.VMEM((plan.hi * plan.block, plan.slots * plan.width), BF16),
            pltpu.VMEM((plan.chunks, plan.slots, plan.width, plan.cols), BF16),
            pltpu.VMEM((plan.chunks, plan.hi, 2, plan.block, plan.cols), F32),
            pltpu.VMEM((plan.chunks, plan.hi, 2, plan.block, plan.cols), BF16),
            pltpu.VMEM((plan.chunks, plan.hi, 2, plan.block, plan.cols), BF16),
            pltpu.VMEM((plan.beams, plan.beams), BF16),
            pltpu.VMEM((2 * plan.block, plan.beams), F32),
            dma((plan.slots,)),
            dma((plan.slots,)),
            dma((plan.chunks, plan.slots)),
            dma((plan.chunks, plan.slots)),
            dma((plan.chunks, plan.hi)),
            dma((plan.chunks, plan.hi)),
        ],
        compiler_params=pltpu.CompilerParams(
            collective_id=0, has_side_effects=True, vmem_limit_bytes=60 * 1024 * 1024
        ),
    )(signal, steer, weights, beam_list.reshape(1, plan.beams))


def solution(mesh):
    placed = (
        P(None, None, ("grp", "sub"), None),
        P(("grp", "sub"), None, None, None),
        P(("grp", "sub"), None, None, None),
        P(),
    )

    def whole(snapshots, steering, combining, beam_list):
        plan = Plan(mesh, snapshots.shape[0], 2 * steering.shape[3], combining.shape[3])
        return jax.shard_map(
            functools.partial(shards, plan),
            mesh=mesh,
            in_specs=placed,
            out_specs=P(None, ("grp", "sub"), None),
            check_vma=False,
        )(snapshots, steering, combining, beam_list)

    return whole
```

```python
import functools

import jax
import jax.numpy as jnp
from jax import lax
from jax.experimental import pallas as pl
from jax.experimental.pallas import tpu as pltpu
from jax.sharding import PartitionSpec as P

MESH = pl.DeviceIdType.MESH
F32 = jnp.float32
BF16 = jnp.bfloat16
LAG = 2


class Plan:
    def __init__(self, mesh, snap, width, beams):
        self.grp = mesh.shape["grp"]
        self.sub = mesh.shape["sub"]
        self.cores = 2 if self.grp % 2 == 0 else 1
        self.nx = self.grp // self.cores
        self.halves, self.pair = (2, 2) if self.sub % 4 == 0 else (1, 1)
        self.hi = self.halves * self.pair
        self.lo = self.sub // self.hi
        self.block = snap // (self.grp * self.sub)
        self.width = width
        self.beams = beams
        self.chunks = 8 if beams % 1024 == 0 else 1
        self.cols = beams // self.chunks
        self.offsets = [(dx, dy) for dx in range(self.nx) for dy in range(self.lo)]
        self.slots = len(self.offsets) * self.cores


def beam_kernel(
    plan,
    x_hbm,
    s_ref,
    w_hbm,
    list_ref,
    out_ref,
    x_ref,
    w_ref,
    in_sem,
    even_buf,
    odd_buf,
    pall,
    pbuf,
    lhs_buf,
    wbuf,
    own_buf,
    share_buf,
    merged_buf,
    got_buf,
    pick_buf,
    acc_buf,
    psend,
    precv,
    wsend,
    wrecv,
    ssend,
    srecv,
):
    cores, nx, lo, hi = plan.cores, plan.nx, plan.lo, plan.hi
    halves, pair = plan.halves, plan.pair
    cols, width, block = plan.cols, plan.width, plan.block
    half = width // 2
    offsets = plan.offsets
    count = len(offsets)
    g = lax.axis_index("grp")
    s = lax.axis_index("sub")
    core, xi = lax.rem(g, cores), lax.div(g, cores)
    z, y = lax.div(s, lo), lax.rem(s, lo)
    zh, zl = lax.div(z, pair), lax.rem(z, pair)

    def peer(dx, dy, dc):
        gg = lax.rem(xi + dx, nx) * cores + lax.rem(core + dc, cores)
        yy = lax.rem(y + dy, lo)
        return gg, yy

    def slot(o, dc):
        return dc * count + o

    plane = [(o, dc) for o in range(count) for dc in range(cores) if (o, dc) != (0, 0)]
    plane.sort(key=lambda item: -sum(1 for v in offsets[item[0]] if v))

    load_w = pltpu.make_async_copy(w_hbm, w_ref, in_sem.at[0])
    load_w.start()
    load_x = pltpu.make_async_copy(x_hbm, x_ref, in_sem.at[1])
    load_x.start()
    barrier = pltpu.get_barrier_semaphore()
    for o, dc in plane:
        gg, yy = peer(*offsets[o], dc)
        pl.semaphore_signal(barrier, inc=1, device_id=(gg, z * lo + yy), device_id_type=MESH)
    if hi > 1:
        near = (g, (2 * zh + 1 - zl) * lo + y)
        far = (g, (2 * (1 - zh) + zl) * lo + y)
        for target in (near, far):
            pl.semaphore_signal(barrier, inc=1, device_id=target, device_id_type=MESH)
    pl.semaphore_wait(barrier, len(plane) + (2 if hi > 1 else 0))

    def w_columns(c):
        return w_ref.at[:, pl.ds(c * cols, cols)]

    sends = []

    def send_w(c):
        for o in sorted(range(count), key=lambda o: -sum(1 for v in offsets[o] if v)):
            if o == 0:
                if cores > 1:
                    gg, yy = peer(0, 0, 1)
                    k = slot(0, 1)
                else:
                    continue
            else:
                gg, yy = peer(*offsets[o], 0)
                k = slot(o, 0)
            copy = pltpu.make_async_remote_copy(
                src_ref=w_columns(c),
                dst_ref=wbuf.at[c, k],
                send_sem=wsend.at[c, k],
                recv_sem=wrecv.at[c, k],
                device_id=(gg, z * lo + yy),
                device_id_type=MESH,
            )
            copy.start()
            sends.append(copy)

    def relay_w(c):
        if cores == 1:
            return
        gg, yy = peer(0, 0, 1)
        for o in range(1, count):
            wait_w(c, slot(o, 0))
            copy = pltpu.make_async_remote_copy(
                src_ref=wbuf.at[c, slot(o, 0)],
                dst_ref=wbuf.at[c, slot(o, 1)],
                send_sem=wsend.at[c, slot(o, 1)],
                recv_sem=wrecv.at[c, slot(o, 1)],
                device_id=(gg, z * lo + yy),
                device_id_type=MESH,
            )
            copy.start()
            sends.append(copy)

    def wait_w(c, k):
        pltpu.make_async_copy(wbuf.at[c, k], wbuf.at[c, k], wrecv.at[c, k]).wait()

    load_w.wait()
    send_w(0)
    load_x.wait()

    upper = s_ref[...]
    lower = jnp.concatenate([-upper[half:], upper[:half]], axis=0)
    rows_g = hi * lo * block
    contract = (((1,), (1,)), ((), ()))
    for gg in range(plan.grp):
        part = x_ref[pl.ds(gg * rows_g * 2, rows_g * 2), :]
        even_buf[...] = lax.dot_general(part, upper, contract, preferred_element_type=F32)
        odd_buf[...] = lax.dot_general(part, lower, contract, preferred_element_type=F32)
        value = even_buf[pl.ds(0, rows_g, stride=2), :] + odd_buf[pl.ds(1, rows_g, stride=2), :]
        pall[gg] = value.reshape(halves, pair, lo, block, width).astype(BF16)

    def half_of(h):
        return zh if h == halves - 1 else 1 - zh

    def send_p(h):
        for o, dc in plane:
            gg, yy = peer(*offsets[o], dc)
            k = slot(o, dc)
            copy = pltpu.make_async_remote_copy(
                src_ref=pall.at[gg, half_of(h), :, yy],
                dst_ref=pbuf.at[h, k],
                send_sem=psend.at[h, k],
                recv_sem=precv.at[h, k],
                device_id=(gg, z * lo + yy),
                device_id_type=MESH,
            )
            copy.start()
            sends.append(copy)

    def wait_p(h):
        own = pall[g, half_of(h), :, y]
        lhs_buf[h, :, pl.ds(0, width)] = own.reshape(pair * block, width)
        for o, dc in reversed(plane):
            k = slot(o, dc)
            pltpu.make_async_copy(pbuf.at[h, k], pbuf.at[h, k], precv.at[h, k]).wait()
            lhs_buf[h, :, pl.ds(k * width, width)] = pbuf[h, k].reshape(pair * block, width)

    send_p(0)
    for c in range(1, 3):
        send_w(c)

    for c in range(plan.chunks):
        row = lax.broadcasted_iota(jnp.int32, (cols, plan.beams), 0) + c * cols
        pick_buf[pl.ds(c * cols, cols), :] = jnp.where(row == list_ref[...], 1.0, 0.0).astype(BF16)
        wbuf[c, 0] = w_ref[:, pl.ds(c * cols, cols)]

    relay_w(0)
    wait_p(0)

    def share(c, k, source, target):
        copy = pltpu.make_async_remote_copy(
            src_ref=source,
            dst_ref=got_buf.at[c, k],
            send_sem=ssend.at[c, k],
            recv_sem=srecv.at[c, k],
            device_id=target,
            device_id_type=MESH,
        )
        copy.start()
        sends.append(copy)

    def wait_share(c, k):
        pltpu.make_async_copy(got_buf.at[c, k], got_buf.at[c, k], srecv.at[c, k]).wait()

    def merge(c):
        if hi == 1:
            return
        wait_share(c, 0)
        merged_buf[c] = (own_buf[0, c, zl] + got_buf[c, 0].astype(F32)).astype(BF16)
        share(c, 2, merged_buf.at[c], far)

    def finish(c):
        total = own_buf[halves - 1, c, zl]
        if hi > 1:
            for k in (1, 2):
                wait_share(c, k)
                total = total + got_buf[c, k].astype(F32)
        rounded = total.astype(BF16).reshape(2 * block, cols)
        placed = jnp.dot(rounded, pick_buf[pl.ds(c * cols, cols), :], preferred_element_type=F32)
        if c == 0:
            acc_buf[...] = placed
        else:
            acc_buf[...] += placed

    def multiply(h, c):
        weights = wbuf[c]
        w_real, w_imag = weights[:, :half], weights[:, half:]
        for part, rhs in enumerate(((w_real, -w_imag), (w_imag, w_real))):
            rhs = jnp.concatenate(rhs, axis=1).reshape(plan.slots * width, cols)
            value = jnp.dot(lhs_buf[h], rhs, preferred_element_type=F32)
            value = value.reshape(pair, block, cols)
            own_buf[h, c, :, part] = value
            share_buf[h, c, :, part] = value.astype(BF16)
        if hi > 1:
            share(c, h, share_buf.at[h, c, 1 - zl], near)

    for c in range(plan.chunks):
        if c + 3 < plan.chunks:
            send_w(c + 3)
        if c == plan.chunks - 3:
            send_p(1)
        for o in range(count):
            if cores > 1:
                wait_w(c, slot(o, 1))
            elif o > 0:
                wait_w(c, slot(o, 0))
        multiply(0, c)
        if c >= LAG:
            merge(c - LAG)
        if c + 1 < plan.chunks:
            relay_w(c + 1)
    for c in range(max(plan.chunks - LAG, 0), plan.chunks):
        merge(c)
    for h in range(1, halves):
        wait_p(h)
        for c in range(plan.chunks):
            multiply(h, c)
    for c in range(plan.chunks):
        finish(c)
    out_ref[...] = acc_buf[...].astype(BF16).reshape(2, block, plan.beams)
    for copy in sends:
        copy.wait_send()


def shards(plan, snapshots, steering, combining, beam_list):
    snap, _, _, elements = snapshots.shape
    signal = snapshots.reshape(snap * 2, elements)
    steer = jnp.transpose(steering[0], (0, 2, 1)).reshape(plan.width, elements)
    weights = combining.reshape(plan.width, plan.beams)
    rows_g = plan.hi * plan.lo * plan.block
    line = (plan.halves, plan.pair)
    vmem = pl.BlockSpec(memory_space=pltpu.VMEM)
    hbm = pl.BlockSpec(memory_space=pl.ANY)
    dma = pltpu.SemaphoreType.DMA
    return pl.pallas_call(
        functools.partial(beam_kernel, plan),
        out_shape=jax.ShapeDtypeStruct((2, plan.block, plan.beams), BF16),
        in_specs=[hbm, vmem, hbm, vmem],
        out_specs=vmem,
        scratch_shapes=[
            pltpu.VMEM(signal.shape, BF16),
            pltpu.VMEM(weights.shape, BF16),
            dma((2,)),
            pltpu.VMEM((rows_g * 2, plan.width), F32),
            pltpu.VMEM((rows_g * 2, plan.width), F32),
            pltpu.VMEM((plan.grp, *line, plan.lo, plan.block, plan.width), BF16),
            pltpu.VMEM((plan.halves, plan.slots, plan.pair, plan.block, plan.width), BF16),
            pltpu.VMEM((plan.halves, plan.pair * plan.block, plan.slots * plan.width), BF16),
            pltpu.VMEM((plan.chunks, plan.slots, plan.width, plan.cols), BF16),
            pltpu.VMEM((plan.halves, plan.chunks, plan.pair, 2, plan.block, plan.cols), F32),
            pltpu.VMEM((plan.halves, plan.chunks, plan.pair, 2, plan.block, plan.cols), BF16),
            pltpu.VMEM((plan.chunks, 2, plan.block, plan.cols), BF16),
            pltpu.VMEM((plan.chunks, 3, 2, plan.block, plan.cols), BF16),
            pltpu.VMEM((plan.beams, plan.beams), BF16),
            pltpu.VMEM((2 * plan.block, plan.beams), F32),
            dma((plan.halves, plan.slots)),
            dma((plan.halves, plan.slots)),
            dma((plan.chunks, plan.slots)),
            dma((plan.chunks, plan.slots)),
            dma((plan.chunks, 3)),
            dma((plan.chunks, 3)),
        ],
        compiler_params=pltpu.CompilerParams(
            collective_id=0, has_side_effects=True, vmem_limit_bytes=60 * 1024 * 1024
        ),
    )(signal, steer, weights, beam_list.reshape(1, plan.beams))


def solution(mesh):
    placed = (
        P(None, None, ("grp", "sub"), None),
        P(("grp", "sub"), None, None, None),
        P(("grp", "sub"), None, None, None),
        P(),
    )

    def whole(snapshots, steering, combining, beam_list):
        plan = Plan(mesh, snapshots.shape[0], 2 * steering.shape[3], combining.shape[3])
        return jax.shard_map(
            functools.partial(shards, plan),
            mesh=mesh,
            in_specs=placed,
            out_specs=P(None, ("grp", "sub"), None),
            check_vma=False,
        )(snapshots, steering, combining, beam_list)

    return whole
```
